128 devices in a mesh: wide: 16 (over y_lo, z, core), narrow: 8 (over y_hi, x).
Axes of the slice: x: 4, y: 4 (y_hi: 2, y_lo: 2; y = y_hi * 2 + y_lo), z: 4, core: 2. Of those that a mesh axis runs over, the one named last changes fastest.
Arguments:
- operator: bfloat16 [16, 8, 2, 2048, 2048], P('wide', 'narrow'), may hold values from -0.125 to 0.125
- sources: bfloat16 [16, 8, 2048, 128], P('wide', 'narrow'), may hold values from -6 to 6
- face_lengths: int32 [16, 8, 4], P('wide', 'narrow'), may hold values from 192 to 640, as said below
Outputs:
- outgoing: bfloat16 [16, 8, 2048, 128], P('wide', 'narrow')
- incoming: bfloat16 [16, 8, 2048, 128], P('wide', 'narrow')
The draws below stay inside these ranges and needn't reach their ends.
Inputs may be any that keep to these rules, and one draw needn't show every extreme that they name: `face_lengths`: the entries of adjacent subdomains for their common face are equal; lower-row and higher-row entries lie in 320 to 640, column entries in 192 to 384.
All inputs are finite; a program needn't handle non-finite values.
Results may differ from the reference program's by a relative error of at most 0.0055.
Values may be sent and summed in bfloat16 or wider, within the bound.
No kernel may reach another device: no remote copies, remote signals or barrier semaphores. Data moves between devices by JAX's collectives and lax.ppermute only.
A program may use at most 64 MiB of HBM per device.

```python
import jax
import jax.numpy as jnp
from jax import lax

FACE_LONG = 640
FACE_SHORT = 384
SOURCES = 64
ITERS = 3
MMAX = 2048
SUB_ROWS = 16
SUB_COLS = 8


def draw_face_lengths(key, part):
    first_key, second_key = jax.random.split(jax.random.fold_in(key, 17))
    longs = jax.random.randint(first_key, (SUB_ROWS + 1, SUB_COLS), FACE_LONG // 2, FACE_LONG + 1)
    shorts = jax.random.randint(second_key, (SUB_ROWS, SUB_COLS + 1), FACE_SHORT // 2, FACE_SHORT + 1)
    longs = longs.at[0, 0].set(FACE_LONG).at[SUB_ROWS, SUB_COLS - 1].set(FACE_LONG // 2)
    shorts = shorts.at[0, 0].set(FACE_SHORT).at[SUB_ROWS - 1, SUB_COLS].set(FACE_SHORT // 2)
    stacked = jnp.stack([longs[:-1], longs[1:], shorts[:, :-1], shorts[:, 1:]], axis=-1)
    return stacked.astype(jnp.int32)


def block_scale(key, shape, pieces, smallest, top_value):
    def one(axis_at, shards_of):
        draws = jax.random.uniform(jax.random.fold_in(jax.random.fold_in(key, 6), axis_at), (shards_of,), jnp.float32, smallest / len(pieces), top_value / len(pieces))
        return jnp.repeat(jnp.exp(draws), shape[axis_at] // shards_of).reshape((-1,) + (1,) * (len(shape) - axis_at - 1))

    loudness = one(*pieces[0])
    for cut in pieces[1:]:
        loudness = loudness * one(*cut)
    return loudness


def centred(key, shape, scale, limit, shards=(), held_as=jnp.bfloat16):
    values = scale * jax.random.normal(key, shape, jnp.float32)
    if shards:
        values = values * block_scale(key, shape, shards, -0.22, 0.18)
    return jnp.clip(values, -limit, limit).astype(held_as)


def setup_inputs(seed: int = 0) -> dict:
    splits = jax.random.split(jax.random.key(seed), 4)
    return {
        "operator": centred(splits[0], (SUB_ROWS, SUB_COLS, 2, MMAX, MMAX), MMAX ** -0.5, 0.125, ((0, 16), (1, 8))),
        "sources": centred(splits[1], (SUB_ROWS, SUB_COLS, MMAX, 2 * SOURCES), 1.0, 6.0, ((0, 16), (1, 8))),
        "face_lengths": draw_face_lengths(jax.random.fold_in(splits[3], 71), 0),
    }


def live_rows(counts):
    total = 2 * FACE_LONG + 2 * FACE_SHORT
    rows = jnp.arange(total, dtype=jnp.int32)
    edges = [0, FACE_LONG, 2 * FACE_LONG, 2 * FACE_LONG + FACE_SHORT]
    live = jnp.zeros((total,), dtype=bool)
    for face in range(4):
        live = live | ((rows >= edges[face]) & (rows < edges[face] + counts[face]))
    return live[:, None]


def trade_all(out):
    low = FACE_LONG
    mid = 2 * FACE_LONG
    high = 2 * FACE_LONG + FACE_SHORT
    lower_face = out[:, :, :low]
    upper_face = out[:, :, low:mid]
    left_face = out[:, :, mid:high]
    right_face = out[:, :, high:]
    zero_row = jnp.zeros_like(upper_face[:1])
    from_lower = jnp.concatenate([zero_row, upper_face[:-1]], axis=0)
    from_upper = jnp.concatenate([lower_face[1:], zero_row], axis=0)
    zero_col = jnp.zeros_like(right_face[:, :1])
    from_left = jnp.concatenate([zero_col, right_face[:, :-1]], axis=1)
    from_right = jnp.concatenate([left_face[:, 1:], zero_col], axis=1)
    return jnp.concatenate([from_lower, from_upper, from_left, from_right], axis=2)


def product(pair):
    oper, field = pair
    total = oper.shape[-1]
    half = field.shape[1] // 2
    stacked = oper.reshape(2 * total, total).astype(jnp.float32)
    both = jnp.dot(stacked, field.astype(jnp.float32), precision=lax.Precision.HIGHEST)
    first = both[:total]
    second = both[total:]
    real_part = first[:, :half] - second[:, half:]
    imag_part = first[:, half:] + second[:, :half]
    return jnp.concatenate([real_part, imag_part], axis=1)


def reference(operator, sources, face_lengths):
    rows_grid, cols_grid = operator.shape[0], operator.shape[1]
    total = operator.shape[-1]
    width = sources.shape[-1]
    count = rows_grid * cols_grid
    live = jax.vmap(live_rows)(face_lengths.reshape(count, 4)).reshape(rows_grid, cols_grid, total, 1)
    masked = jnp.where(live, sources, jnp.zeros_like(sources))
    incoming = trade_all(masked)
    oper_flat = operator.reshape(count, 2, total, total)
    outgoing = masked
    for step in range(ITERS):
        terms = lax.map(product, (oper_flat, incoming.reshape(count, total, width)))
        terms = terms.reshape(rows_grid, cols_grid, total, width) + sources.astype(jnp.float32)
        outgoing = jnp.where(live, terms, jnp.zeros_like(terms)).astype(jnp.bfloat16)
        incoming = trade_all(outgoing)
    return outgoing, incoming
```

```python
import jax
import jax.numpy as jnp
from jax import lax
from jax.experimental import pallas as pl
from jax.experimental.pallas import tpu as pltpu
from jax.sharding import PartitionSpec as P


FACE_LONG = 640
FACE_SHORT = 384
WIDE = 2 * FACE_LONG
NARROW = 2 * FACE_SHORT
TOTAL = WIDE + NARROW
WIDTH = 128
HALF = WIDTH // 2
ITERS = 3
BLOCK = 256
LOADS = 16

VMEM = pl.BlockSpec(memory_space=pltpu.VMEM)
SMEM = pl.BlockSpec(memory_space=pltpu.SMEM)
ANY = pl.BlockSpec(memory_space=pl.ANY)
BF16 = jnp.bfloat16
F32 = jnp.float32


def kept(shape, dtype):
    return pltpu.VMEM(shape, dtype)


def held(value):
    return pltpu.with_memory_space_constraint(value, pltpu.VMEM)


def call(kernel, out, specs, flops, out_specs=None):
    return pl.pallas_call(
        kernel,
        out_shape=out,
        in_specs=specs,
        out_specs=VMEM if out_specs is None else out_specs,
        cost_estimate=pl.CostEstimate(flops=flops, bytes_accessed=flops // 128, transcendentals=0),
        compiler_params=pltpu.CompilerParams(vmem_limit_bytes=16 * 1024 * 1024),
    )


def shifted(value, axis, steps):
    count = lax.axis_size(axis)
    return lax.ppermute(value, axis, [(i, (i + steps) % count) for i in range(count)])


def prepare(counts_ref, sources_ref, kept_ref, live_ref, inside_ref, lower_ref, upper_ref, left_ref, right_ref):
    row, col = lax.axis_index("wide"), lax.axis_index("narrow")
    rows, cols = lax.axis_size("wide"), lax.axis_size("narrow")
    bounded = (row > 0, row < rows - 1, col > 0, col < cols - 1)
    kept_ref[...] = sources_ref[0, 0]
    base = 0
    for face, (size, out_ref) in enumerate(
        ((FACE_LONG, lower_ref), (FACE_LONG, upper_ref), (FACE_SHORT, left_ref), (FACE_SHORT, right_ref))
    ):
        count = counts_ref[0, 0, face]
        slots = lax.broadcasted_iota(jnp.int32, (size, WIDTH), 0)
        live_ref[base : base + size] = jnp.where(slots < count, 1.0, 0.0).astype(BF16)
        inner = jnp.where(bounded[face], count, 0)
        inside_ref[base : base + size] = jnp.where(slots < inner, 1.0, 0.0).astype(BF16)
        out_ref[...] = sources_ref[0, 0, base : base + size]
        base += size


def load(operator_ref, out_ref, sems):
    rows = TOTAL // LOADS
    copies = []
    for part in range(2):
        for i in range(LOADS):
            at = pl.ds(i * rows, rows)
            copies.append(
                pltpu.make_async_copy(operator_ref.at[0, 0, part, at], out_ref.at[part, at], sems.at[part * LOADS + i])
            )
    for copy in copies:
        copy.start()
    for copy in copies:
        copy.wait()


def masked(value, mask):
    return jnp.where(mask != 0, value, jnp.zeros_like(value))


def turned(field):
    return jnp.concatenate([-field[:, HALF:], field[:, :HALF]], axis=1)


def terms(op_ref, rows, columns, field, turn):
    first = jnp.dot(op_ref[0, rows, columns], field, preferred_element_type=F32)
    second = jnp.dot(op_ref[1, rows, columns], turn, preferred_element_type=F32)
    return first + second


def from_wide(op_ref, sources_ref, inside_ref, lower_ref, upper_ref, wide_ref, narrow_ref):
    field = jnp.concatenate([lower_ref[...], upper_ref[...]], axis=0)
    field = masked(field, inside_ref[:WIDE])
    turn = turned(field)
    for base in range(0, TOTAL, BLOCK):
        rows = slice(base, base + BLOCK)
        total = terms(op_ref, rows, slice(0, WIDE), field, turn) + sources_ref[rows].astype(F32)
        if base < WIDE:
            wide_ref[base : base + BLOCK] = total
        else:
            narrow_ref[base - WIDE : base - WIDE + BLOCK] = total


def narrow_field(inside_ref, left_ref, right_ref):
    field = jnp.concatenate([left_ref[...], right_ref[...]], axis=0)
    return masked(field, inside_ref[WIDE:])


def from_narrow(op_ref, live_ref, inside_ref, left_ref, right_ref, sum_ref, outs, start, size):
    field = narrow_field(inside_ref, left_ref, right_ref)
    turn = turned(field)
    for side, out_ref in enumerate(outs):
        for base in range(0, size, 128):
            rows = slice(start + side * size + base, start + side * size + base + 128)
            at = slice(side * size + base, side * size + base + 128)
            total = terms(op_ref, rows, slice(WIDE, TOTAL), field, turn) + sum_ref[at]
            out_ref[base : base + 128] = masked(total, live_ref[rows]).astype(BF16)


def narrow_rows(op_ref, live_ref, inside_ref, left_ref, right_ref, sum_ref, out_left_ref, out_right_ref):
    outs = (out_left_ref, out_right_ref)
    from_narrow(op_ref, live_ref, inside_ref, left_ref, right_ref, sum_ref, outs, WIDE, FACE_SHORT)


def wide_rows(op_ref, live_ref, inside_ref, left_ref, right_ref, sum_ref, out_lower_ref, out_upper_ref):
    outs = (out_lower_ref, out_upper_ref)
    from_narrow(op_ref, live_ref, inside_ref, left_ref, right_ref, sum_ref, outs, 0, FACE_LONG)


def joined(lower_ref, upper_ref, left_ref, right_ref, out_ref):
    base = 0
    for ref in (lower_ref, upper_ref, left_ref, right_ref):
        out_ref[0, 0, base : base + ref.shape[0]] = ref[...]
        base += ref.shape[0]


def joined_inside(inside_ref, lower_ref, upper_ref, left_ref, right_ref, out_ref):
    base = 0
    for ref in (lower_ref, upper_ref, left_ref, right_ref):
        rows = slice(base, base + ref.shape[0])
        out_ref[0, 0, rows] = masked(ref[...], inside_ref[rows])
        base += ref.shape[0]


def body(operator, sources, face_lengths):
    long, short = (FACE_LONG, WIDTH), (FACE_SHORT, WIDTH)
    faces = [kept(long, BF16), kept(long, BF16), kept(short, BF16), kept(short, BF16)]
    whole = kept((TOTAL, WIDTH), BF16)
    source, live, inside, lower, upper, left, right = call(
        prepare, [whole, whole, whole] + faces, [SMEM, VMEM], 1 << 20, [VMEM] * 7
    )(face_lengths, sources)
    in_left, in_right = shifted(right, "narrow", 1), shifted(left, "narrow", -1)
    in_lower, in_upper = shifted(upper, "wide", 1), shifted(lower, "wide", -1)
    oper = pl.pallas_call(
        load,
        out_shape=kept((2, TOTAL, TOTAL), BF16),
        in_specs=[ANY],
        out_specs=VMEM,
        scratch_shapes=[pltpu.SemaphoreType.DMA((2 * LOADS,))],
        cost_estimate=pl.CostEstimate(flops=1 << 33, bytes_accessed=1 << 24, transcendentals=0),
        compiler_params=pltpu.CompilerParams(vmem_limit_bytes=16 * 1024 * 1024),
        name="load",
    )(pltpu.with_memory_space_constraint(operator, pltpu.HBM))
    oper, source, live, inside = map(held, (oper, source, live, inside))
    unit = 2 * 2 * WIDTH
    for _ in range(ITERS):
        wide_sum, narrow_sum = call(
            from_wide,
            [kept((WIDE, WIDTH), F32), kept((NARROW, WIDTH), F32)],
            [VMEM] * 5,
            unit * TOTAL * WIDE,
            [VMEM] * 2,
        )(oper, source, inside, held(in_lower), held(in_upper))
        in_left, in_right = held(in_left), held(in_right)
        left, right = call(
            narrow_rows, [kept(short, BF16)] * 2, [VMEM] * 6, unit * NARROW * NARROW, [VMEM] * 2
        )(oper, live, inside, in_left, in_right, held(narrow_sum))
        next_left = shifted(right, "narrow", 1)
        next_right = shifted(left, "narrow", -1)
        lower, upper = call(
            wide_rows, [kept(long, BF16)] * 2, [VMEM] * 6, unit * NARROW * WIDE, [VMEM] * 2
        )(oper, live, inside, in_left, in_right, held(wide_sum))
        in_lower, in_upper = shifted(upper, "wide", 1), shifted(lower, "wide", -1)
        in_left, in_right = next_left, next_right
    result = jax.ShapeDtypeStruct((1, 1, TOTAL, WIDTH), BF16)
    outgoing = call(joined, result, [VMEM] * 4, 1 << 26)(*map(held, (lower, upper, left, right)))
    incoming = call(joined_inside, result, [VMEM] * 5, 1 << 20)(
        inside, *map(held, (in_lower, in_upper, in_left, in_right))
    )
    return (outgoing, incoming)


def solution(mesh):
    in_specs = (
        P("wide", "narrow", None, None, None),
        P("wide", "narrow", None, None),
        P("wide", "narrow", None),
    )
    out_specs = (P("wide", "narrow", None, None), P("wide", "narrow", None, None))
    return jax.shard_map(body, mesh=mesh, in_specs=in_specs, out_specs=out_specs, check_vma=False)
```

```python
import jax
import jax.numpy as jnp
from jax import lax
from jax.experimental import pallas as pl
from jax.experimental.pallas import tpu as pltpu
from jax.sharding import PartitionSpec as P


FACE_LONG = 640
FACE_SHORT = 384
WIDE = 2 * FACE_LONG
NARROW = 2 * FACE_SHORT
TOTAL = WIDE + NARROW
WIDTH = 128
HALF = WIDTH // 2
ITERS = 3
BLOCK = 256
SLOTS = 4
FACES = ((0, FACE_LONG), (FACE_LONG, FACE_LONG), (WIDE, FACE_SHORT), (WIDE + FACE_SHORT, FACE_SHORT))

VMEM = pl.BlockSpec(memory_space=pltpu.VMEM)
ANY = pl.BlockSpec(memory_space=pl.ANY)
BF16 = jnp.bfloat16
F32 = jnp.float32
LONG = pltpu.VMEM((WIDTH, FACE_LONG), BF16)
SHORT = pltpu.VMEM((WIDTH, FACE_SHORT), BF16)
WHOLE = pltpu.VMEM((WIDTH, TOTAL), BF16)
ACROSS = (((1,), (1,)), ((), ()))


def held(value):
    return pltpu.with_memory_space_constraint(value, pltpu.VMEM)


def stored(value):
    return pltpu.with_memory_space_constraint(value, pltpu.HBM)


def call(kernel, out, specs, flops, scratch=()):
    return pl.pallas_call(
        kernel,
        out_shape=out,
        in_specs=specs,
        out_specs=[VMEM] * len(out),
        scratch_shapes=scratch,
        cost_estimate=pl.CostEstimate(flops=flops, bytes_accessed=flops // 128, transcendentals=0),
        compiler_params=pltpu.CompilerParams(vmem_limit_bytes=12 * 1024 * 1024),
    )


def pairing(axis, offset, rows, cols):
    pairs = []
    for row in range(rows):
        for col in range(cols):
            at, count = (row, rows) if axis == "wide" else (col, cols)
            other = ((at - offset) ^ 1) + offset
            inside = 0 <= other < count
            if axis == "wide":
                to = (other, col) if inside else (row, col ^ 1)
            else:
                to = (row, other) if inside else (row ^ 1, col)
            pairs.append((row * cols + col, to[0] * cols + to[1]))
    return pairs


def swap(value, axis, offset):
    pairs = pairing(axis, offset, lax.axis_size("wide"), lax.axis_size("narrow"))
    return lax.ppermute(value, ("wide", "narrow"), pairs)


def swap_all(faces):
    wide_first, wide_second, narrow_first, narrow_second = faces
    narrow_second = swap(narrow_second, "narrow", 1)
    narrow_first = swap(narrow_first, "narrow", 0)
    wide_second = swap(wide_second, "wide", 1)
    wide_first = swap(wide_first, "wide", 0)
    return wide_first, wide_second, narrow_first, narrow_second


def even(axis):
    return lax.rem(lax.axis_index(axis), 2) == 0


def crossed(axis, first, second):
    flag = even(axis)
    return jnp.where(flag, second, first), jnp.where(flag, first, second)


def identity(size):
    rows = lax.broadcasted_iota(jnp.int32, (size, size), 0)
    columns = lax.broadcasted_iota(jnp.int32, (size, size), 1)
    return jnp.where(rows == columns, 1.0, 0.0).astype(BF16)


def masked(value, mask):
    return jnp.where(mask != 0, value, jnp.zeros_like(value))


def prepare(counts_ref, sources_ref, kept_ref, live_ref, inside_ref, wf_ref, ws_ref, nf_ref, ns_ref, counts, rows, sems):
    copies = (
        pltpu.make_async_copy(counts_ref, counts, sems.at[0]),
        pltpu.make_async_copy(sources_ref.at[0, 0], rows, sems.at[1]),
    )
    for copy in copies:
        copy.start()
    row, col = lax.axis_index("wide"), lax.axis_index("narrow")
    bounded = (row > 0, row < lax.axis_size("wide") - 1, col > 0, col < lax.axis_size("narrow") - 1)
    copies[0].wait()
    for face, (base, size) in enumerate(FACES):
        count = counts[0, 0, face]
        slots = lax.broadcasted_iota(jnp.int32, (WIDTH, size), 1)
        live_ref[:, base : base + size] = jnp.where(slots < count, 1.0, 0.0).astype(BF16)
        inner = jnp.where(bounded[face], count, 0)
        inside_ref[:, base : base + size] = jnp.where(slots < inner, 1.0, 0.0).astype(BF16)
    copies[1].wait()
    flipped = lax.dot_general(identity(WIDTH), rows[...], ACROSS, preferred_element_type=F32).astype(BF16)
    kept_ref[...] = flipped
    faces = [flipped[:, base : base + size] for base, size in FACES]
    wf_ref[...], ws_ref[...] = crossed("wide", faces[0], faces[1])
    nf_ref[...], ns_ref[...] = crossed("narrow", faces[2], faces[3])


def load(operator_ref, out_ref, slots, sems):
    blocks = TOTAL // BLOCK
    unit = identity(BLOCK)

    def fetch(i):
        part, block = divmod(i, blocks)
        at = operator_ref.at[0, 0, part, pl.ds(block * BLOCK, BLOCK)]
        return pltpu.make_async_copy(at, slots.at[i % SLOTS], sems.at[i % SLOTS])

    for i in range(SLOTS):
        fetch(i).start()
    for i in range(2 * blocks):
        fetch(i).wait()
        part, block = divmod(i, blocks)
        at = slice(block * BLOCK, (block + 1) * BLOCK)
        for base in range(0, TOTAL, BLOCK):
            tile = slots[i % SLOTS, :, base : base + BLOCK]
            turned = lax.dot_general(unit, tile, ACROSS, preferred_element_type=F32)
            out_ref[part, base : base + BLOCK, at] = turned.astype(BF16)
        if i + SLOTS < 2 * blocks:
            fetch(i + SLOTS).start()


def received(axis, first_ref, second_ref, mask):
    lower, higher = crossed(axis, first_ref[...], second_ref[...])
    return masked(jnp.concatenate([lower, higher], axis=1), mask)


def terms(op_ref, rows, columns, field):
    turn = jnp.concatenate([-field[HALF:], field[:HALF]], axis=0)
    first = jnp.dot(field, op_ref[0, rows, columns], preferred_element_type=F32)
    return first + jnp.dot(turn, op_ref[1, rows, columns], preferred_element_type=F32)


def from_wide(op_ref, kept_ref, inside_ref, first_ref, second_ref, sum_ref):
    field = received("wide", first_ref, second_ref, inside_ref[:, :WIDE])
    for base in range(0, TOTAL, BLOCK):
        at = slice(base, base + BLOCK)
        sum_ref[:, at] = terms(op_ref, slice(0, WIDE), at, field) + kept_ref[:, at].astype(F32)


def finish(op_ref, live_ref, inside_ref, first_ref, second_ref, sum_ref, wf_ref, ws_ref, nf_ref, ns_ref, *result):
    field = received("narrow", first_ref, second_ref, inside_ref[:, WIDE:])
    faces = []
    for base, size in FACES:
        at = slice(base, base + size)
        total = terms(op_ref, slice(WIDE, TOTAL), at, field) + sum_ref[:, at]
        faces.append(masked(total.astype(BF16), live_ref[:, at]))
    wf_ref[...], ws_ref[...] = crossed("wide", faces[0], faces[1])
    nf_ref[...], ns_ref[...] = crossed("narrow", faces[2], faces[3])


def put(out_ref, value):
    unit = identity(BLOCK)
    for base in range(0, TOTAL, BLOCK):
        rows = lax.dot_general(unit, value[:, base : base + BLOCK], ACROSS, preferred_element_type=F32)
        out_ref[0, 0, base : base + BLOCK] = rows.astype(BF16)


def emit_outgoing(wf_ref, ws_ref, nf_ref, ns_ref, out_ref):
    pieces = crossed("wide", wf_ref[...], ws_ref[...]) + crossed("narrow", nf_ref[...], ns_ref[...])
    put(out_ref, jnp.concatenate(pieces, axis=1))


def emit_incoming(inside_ref, wf_ref, ws_ref, nf_ref, ns_ref, out_ref):
    pieces = crossed("wide", wf_ref[...], ws_ref[...]) + crossed("narrow", nf_ref[...], ns_ref[...])
    put(out_ref, masked(jnp.concatenate(pieces, axis=1), inside_ref[...]))


def body(operator, sources, face_lengths):
    faces = [LONG, LONG, SHORT, SHORT]
    unit = 2 * 2 * WIDTH
    scratch = [pltpu.SMEM((1, 1, 4), jnp.int32), pltpu.VMEM((TOTAL, WIDTH), BF16), pltpu.SemaphoreType.DMA((2,))]
    kept, live, inside, *out = call(prepare, [WHOLE] * 3 + faces, [ANY, ANY], 1 << 20, scratch)(
        stored(face_lengths), stored(sources)
    )
    into = swap_all(out)
    scratch = [pltpu.VMEM((SLOTS, BLOCK, TOTAL), BF16), pltpu.SemaphoreType.DMA((SLOTS,))]
    (oper,) = call(load, [pltpu.VMEM((2, TOTAL, TOTAL), BF16)], [ANY], 1 << 33, scratch)(stored(operator))
    oper, kept, live, inside = map(held, (oper, kept, live, inside))
    for _ in range(ITERS):
        wf, ws, nf, ns = map(held, into)
        (total,) = call(
            from_wide, [pltpu.VMEM((WIDTH, TOTAL), F32)], [VMEM] * 5, unit * TOTAL * WIDE
        )(oper, kept, inside, wf, ws)
        out = call(finish, faces, [VMEM] * 6, unit * TOTAL * NARROW)(oper, live, inside, nf, ns, held(total))
        into = swap_all(out)
    result = [jax.ShapeDtypeStruct((1, 1, TOTAL, WIDTH), BF16)]
    (outgoing,) = call(emit_outgoing, result, [VMEM] * 4, 1 << 26)(*map(held, out))
    (incoming,) = call(emit_incoming, result, [VMEM] * 5, 1 << 20)(inside, *map(held, into))
    return (outgoing, incoming)


def solution(mesh):
    in_specs = (
        P("wide", "narrow", None, None, None),
        P("wide", "narrow", None, None),
        P("wide", "narrow", None),
    )
    out_specs = (P("wide", "narrow", None, None), P("wide", "narrow", None, None))
    return jax.shard_map(body, mesh=mesh, in_specs=in_specs, out_specs=out_specs, check_vma=False)
```

```python
import jax
import jax.numpy as jnp
from jax import lax
from jax.experimental import pallas as pl
from jax.experimental.pallas import tpu as pltpu
from jax.sharding import PartitionSpec as P


FACE_LONG = 640
FACE_SHORT = 384
WIDE = 2 * FACE_LONG
NARROW = 2 * FACE_SHORT
TOTAL = WIDE + NARROW
WIDTH = 128
HALF = WIDTH // 2
ITERS = 3
BLOCK = 256
FACES = ((0, FACE_LONG), (FACE_LONG, FACE_LONG), (WIDE, FACE_SHORT), (WIDE + FACE_SHORT, FACE_SHORT))

VMEM = pl.BlockSpec(memory_space=pltpu.VMEM)
ANY = pl.BlockSpec(memory_space=pl.ANY)
BF16 = jnp.bfloat16
F32 = jnp.float32
LONG = pltpu.VMEM((WIDTH, FACE_LONG), BF16)
SHORT = pltpu.VMEM((WIDTH, FACE_SHORT), BF16)
WHOLE = pltpu.VMEM((WIDTH, TOTAL), BF16)
ACROSS = (((1,), (1,)), ((), ()))


def held(value):
    return pltpu.with_memory_space_constraint(value, pltpu.VMEM)


def stored(value):
    return pltpu.with_memory_space_constraint(value, pltpu.HBM)


def call(kernel, out, specs, flops, scratch=(), place=VMEM):
    return pl.pallas_call(
        kernel,
        out_shape=out,
        in_specs=specs,
        out_specs=[place] * len(out),
        scratch_shapes=scratch,
        cost_estimate=pl.CostEstimate(flops=flops, bytes_accessed=flops // 128, transcendentals=0),
        compiler_params=pltpu.CompilerParams(vmem_limit_bytes=12 * 1024 * 1024),
    )


def pairing(axis, offset, rows, cols):
    pairs = []
    for row in range(rows):
        for col in range(cols):
            at, count = (row, rows) if axis == "wide" else (col, cols)
            other = ((at - offset) ^ 1) + offset
            inside = 0 <= other < count
            if axis == "wide":
                to = (other, col) if inside else (row, col ^ 1)
            else:
                to = (row, other) if inside else (row ^ 1, col)
            pairs.append((row * cols + col, to[0] * cols + to[1]))
    return pairs


def swap(value, axis, offset):
    pairs = pairing(axis, offset, lax.axis_size("wide"), lax.axis_size("narrow"))
    return lax.ppermute(value, ("wide", "narrow"), pairs)


def swap_all(faces):
    wide_first, wide_second, narrow_first, narrow_second = faces
    narrow_second = swap(narrow_second, "narrow", 1)
    narrow_first = swap(narrow_first, "narrow", 0)
    wide_second = swap(wide_second, "wide", 1)
    wide_first = swap(wide_first, "wide", 0)
    return wide_first, wide_second, narrow_first, narrow_second


def even(axis):
    return lax.rem(lax.axis_index(axis), 2) == 0


def crossed(axis, first, second):
    flag = even(axis)
    return jnp.where(flag, second, first), jnp.where(flag, first, second)


def identity(size):
    rows = lax.broadcasted_iota(jnp.int32, (size, size), 0)
    columns = lax.broadcasted_iota(jnp.int32, (size, size), 1)
    return jnp.where(rows == columns, 1.0, 0.0).astype(BF16)


def masked(value, mask):
    return jnp.where(mask != 0, value, jnp.zeros_like(value))


def prepare(counts_ref, sources_ref, kept_ref, live_ref, inside_ref, wf_ref, ws_ref, nf_ref, ns_ref, counts, rows, sems):
    copies = (
        pltpu.make_async_copy(counts_ref, counts, sems.at[0]),
        pltpu.make_async_copy(sources_ref.at[0, 0], rows, sems.at[1]),
    )
    for copy in copies:
        copy.start()
    row, col = lax.axis_index("wide"), lax.axis_index("narrow")
    bounded = (row > 0, row < lax.axis_size("wide") - 1, col > 0, col < lax.axis_size("narrow") - 1)
    copies[0].wait()
    for face, (base, size) in enumerate(FACES):
        count = counts[0, 0, face]
        slots = lax.broadcasted_iota(jnp.int32, (WIDTH, size), 1)
        live_ref[:, base : base + size] = jnp.where(slots < count, 1.0, 0.0).astype(BF16)
        inner = jnp.where(bounded[face], count, 0)
        inside_ref[:, base : base + size] = jnp.where(slots < inner, 1.0, 0.0).astype(BF16)
    copies[1].wait()
    flipped = lax.dot_general(identity(WIDTH), rows[...], ACROSS, preferred_element_type=F32).astype(BF16)
    kept_ref[...] = flipped
    faces = [flipped[:, base : base + size] for base, size in FACES]
    wf_ref[...], ws_ref[...] = crossed("wide", faces[0], faces[1])
    nf_ref[...], ns_ref[...] = crossed("narrow", faces[2], faces[3])


def turn(operator_ref, out_ref):
    unit = identity(BLOCK)
    for part in range(2):
        for low in range(0, TOTAL, BLOCK):
            for base in range(0, TOTAL, BLOCK):
                tile = operator_ref[0, 0, part, low : low + BLOCK, base : base + BLOCK]
                turned = lax.dot_general(unit, tile, ACROSS, preferred_element_type=F32)
                out_ref[part, base : base + BLOCK, low : low + BLOCK] = turned.astype(BF16)


def received(axis, first_ref, second_ref, mask):
    lower, higher = crossed(axis, first_ref[...], second_ref[...])
    return masked(jnp.concatenate([lower, higher], axis=1), mask)


def terms(op_ref, rows, columns, field):
    turn = jnp.concatenate([-field[HALF:], field[:HALF]], axis=0)
    first = jnp.dot(field, op_ref[0, rows, columns], preferred_element_type=F32)
    return first + jnp.dot(turn, op_ref[1, rows, columns], preferred_element_type=F32)


def from_wide(op_ref, kept_ref, inside_ref, first_ref, second_ref, sum_ref):
    field = received("wide", first_ref, second_ref, inside_ref[:, :WIDE])
    for base in range(0, TOTAL, BLOCK):
        at = slice(base, base + BLOCK)
        sum_ref[:, at] = terms(op_ref, slice(0, WIDE), at, field) + kept_ref[:, at].astype(F32)


def narrow_base(first):
    base = jnp.where(even("narrow") == first, WIDE + FACE_SHORT, WIDE)
    return pl.multiple_of(base, 128)


def narrow_terms(op_ref, base, columns, field):
    turn = jnp.concatenate([-field[HALF:], field[:HALF]], axis=0)
    head, tail = pl.ds(base, BLOCK), pl.ds(pl.multiple_of(base + BLOCK, 128), FACE_SHORT - BLOCK)
    total = jnp.dot(field[:, :BLOCK], op_ref[0, head, columns], preferred_element_type=F32)
    total += jnp.dot(turn[:, :BLOCK], op_ref[1, head, columns], preferred_element_type=F32)
    both = jnp.concatenate([field[:, BLOCK:], turn[:, BLOCK:]], axis=1)
    rest = jnp.concatenate([op_ref[0, tail, columns], op_ref[1, tail, columns]], axis=0)
    return total + jnp.dot(both, rest, preferred_element_type=F32)


def from_first(op_ref, inside_ref, narrow_ref, before_ref, sum_ref):
    base = narrow_base(True)
    side = masked(narrow_ref[...], inside_ref[:, pl.ds(base, FACE_SHORT)])
    for start in range(0, TOTAL, BLOCK):
        at = slice(start, start + BLOCK)
        sum_ref[:, at] = narrow_terms(op_ref, base, at, side) + before_ref[:, at]


def finish(op_ref, live_ref, inside_ref, narrow_ref, sum_ref, wf_ref, ws_ref, nf_ref, ns_ref):
    base = narrow_base(False)
    side = masked(narrow_ref[...], inside_ref[:, pl.ds(base, FACE_SHORT)])
    faces = []
    for start, size in FACES:
        at = slice(start, start + size)
        total = narrow_terms(op_ref, base, at, side) + sum_ref[:, at]
        faces.append(masked(total.astype(BF16), live_ref[:, at]))
    wf_ref[...], ws_ref[...] = crossed("wide", faces[0], faces[1])
    nf_ref[...], ns_ref[...] = crossed("narrow", faces[2], faces[3])


def put(out_ref, rows_ref, sems, value):
    unit = identity(BLOCK)
    copies = []
    for i, base in enumerate(range(0, TOTAL, BLOCK)):
        rows = lax.dot_general(unit, value[:, base : base + BLOCK], ACROSS, preferred_element_type=F32)
        rows_ref[base : base + BLOCK] = rows.astype(BF16)
        at = pl.ds(base, BLOCK)
        copies.append(pltpu.make_async_copy(rows_ref.at[at], out_ref.at[0, 0, at], sems.at[i]))
        copies[-1].start()
    for copy in copies:
        copy.wait()


def emit_outgoing(wf_ref, ws_ref, nf_ref, ns_ref, out_ref, rows_ref, sems):
    pieces = crossed("wide", wf_ref[...], ws_ref[...]) + crossed("narrow", nf_ref[...], ns_ref[...])
    put(out_ref, rows_ref, sems, jnp.concatenate(pieces, axis=1))


def emit_incoming(inside_ref, wf_ref, ws_ref, nf_ref, ns_ref, out_ref, rows_ref, sems):
    pieces = crossed("wide", wf_ref[...], ws_ref[...]) + crossed("narrow", nf_ref[...], ns_ref[...])
    put(out_ref, rows_ref, sems, masked(jnp.concatenate(pieces, axis=1), inside_ref[...]))


def body(operator, sources, face_lengths):
    faces = [LONG, LONG, SHORT, SHORT]
    unit = 2 * 2 * WIDTH
    scratch = [pltpu.SMEM((1, 1, 4), jnp.int32), pltpu.VMEM((TOTAL, WIDTH), BF16), pltpu.SemaphoreType.DMA((2,))]
    kept, live, inside, *out = call(prepare, [WHOLE] * 3 + faces, [ANY, ANY], 1 << 34, scratch)(
        stored(face_lengths), stored(sources)
    )
    into = swap_all(out)
    (oper,) = call(turn, [pltpu.VMEM((2, TOTAL, TOTAL), BF16)], [VMEM], 1 << 33)(held(operator))
    oper, kept, live, inside = map(held, (oper, kept, live, inside))
    for _ in range(ITERS):
        wf, ws, nf, ns = map(held, into)
        (total,) = call(
            from_wide, [pltpu.VMEM((WIDTH, TOTAL), F32)], [VMEM] * 5, unit * TOTAL * WIDE
        )(oper, kept, inside, wf, ws)
        (total,) = call(
            from_first, [pltpu.VMEM((WIDTH, TOTAL), F32)], [VMEM] * 4, unit * TOTAL * FACE_SHORT
        )(oper, inside, nf, held(total))
        out = call(finish, faces, [VMEM] * 5, unit * TOTAL * FACE_SHORT)(oper, live, inside, ns, held(total))
        into = swap_all(out)
    scratch = [pltpu.VMEM((TOTAL, WIDTH), BF16), pltpu.SemaphoreType.DMA((TOTAL // BLOCK,))]
    result = [jax.ShapeDtypeStruct((1, 1, TOTAL, WIDTH), BF16)]
    (outgoing,) = call(emit_outgoing, result, [VMEM] * 4, 1 << 26, scratch, ANY)(*map(held, out))
    (incoming,) = call(emit_incoming, result, [VMEM] * 5, 1 << 20, scratch, ANY)(inside, *map(held, into))
    return (outgoing, incoming)


def solution(mesh):
    in_specs = (
        P("wide", "narrow", None, None, None),
        P("wide", "narrow", None, None),
        P("wide", "narrow", None),
    )
    out_specs = (P("wide", "narrow", None, None), P("wide", "narrow", None, None))
    return jax.shard_map(body, mesh=mesh, in_specs=in_specs, out_specs=out_specs, check_vma=False)
```

```python
import jax
import jax.numpy as jnp
from jax import lax
from jax.experimental import pallas as pl
from jax.experimental.pallas import tpu as pltpu
from jax.sharding import PartitionSpec as P


FACE_LONG = 640
FACE_SHORT = 384
WIDE = 2 * FACE_LONG
NARROW = 2 * FACE_SHORT
TOTAL = WIDE + NARROW
WIDTH = 128
HALF = WIDTH // 2
ITERS = 3
BLOCK = 256
FACES = ((0, FACE_LONG), (FACE_LONG, FACE_LONG), (WIDE, FACE_SHORT), (WIDE + FACE_SHORT, FACE_SHORT))

VMEM = pl.BlockSpec(memory_space=pltpu.VMEM)
ANY = pl.BlockSpec(memory_space=pl.ANY)
BF16 = jnp.bfloat16
F32 = jnp.float32
LONG = pltpu.VMEM((WIDTH, FACE_LONG), BF16)
SHORT = pltpu.VMEM((WIDTH, FACE_SHORT), BF16)
WHOLE = pltpu.VMEM((WIDTH, TOTAL), BF16)
ACROSS = (((1,), (1,)), ((), ()))


def held(value):
    return pltpu.with_memory_space_constraint(value, pltpu.VMEM)


def stored(value):
    return pltpu.with_memory_space_constraint(value, pltpu.HBM)


def call(kernel, out, specs, flops, scratch=(), place=VMEM):
    return pl.pallas_call(
        kernel,
        out_shape=out,
        in_specs=specs,
        out_specs=[place] * len(out),
        scratch_shapes=scratch,
        cost_estimate=pl.CostEstimate(flops=flops, bytes_accessed=flops // 128, transcendentals=0),
        compiler_params=pltpu.CompilerParams(vmem_limit_bytes=12 * 1024 * 1024),
    )


def pairing(axis, offset, rows, cols):
    pairs = []
    for row in range(rows):
        for col in range(cols):
            at, count = (row, rows) if axis == "wide" else (col, cols)
            other = ((at - offset) ^ 1) + offset
            inside = 0 <= other < count
            if axis == "wide":
                to = (other, col) if inside else (row, col ^ 1)
            else:
                to = (row, other) if inside else (row ^ 1, col)
            pairs.append((row * cols + col, to[0] * cols + to[1]))
    return pairs


def swap(value, axis, offset):
    pairs = pairing(axis, offset, lax.axis_size("wide"), lax.axis_size("narrow"))
    return lax.ppermute(value, ("wide", "narrow"), pairs)


def swap_all(faces):
    wide_first, wide_second, narrow_first, narrow_second = faces
    narrow_second = swap(narrow_second, "narrow", 1)
    narrow_first = swap(narrow_first, "narrow", 0)
    wide_second = swap(wide_second, "wide", 1)
    wide_first = swap(wide_first, "wide", 0)
    return wide_first, wide_second, narrow_first, narrow_second


def even(axis):
    return lax.rem(lax.axis_index(axis), 2) == 0


def crossed(axis, first, second):
    flag = even(axis)
    return jnp.where(flag, second, first), jnp.where(flag, first, second)


def identity(size):
    rows = lax.broadcasted_iota(jnp.int32, (size, size), 0)
    columns = lax.broadcasted_iota(jnp.int32, (size, size), 1)
    return jnp.where(rows == columns, 1.0, 0.0).astype(BF16)


def masked(value, mask):
    return jnp.where(mask != 0, value, jnp.zeros_like(value))


def prepare(counts_ref, sources_ref, kept_ref, live_ref, inside_ref, wf_ref, ws_ref, nf_ref, ns_ref, counts, rows, sems):
    copies = (
        pltpu.make_async_copy(counts_ref, counts, sems.at[0]),
        pltpu.make_async_copy(sources_ref.at[0, 0], rows, sems.at[1]),
    )
    for copy in copies:
        copy.start()
    row, col = lax.axis_index("wide"), lax.axis_index("narrow")
    bounded = (row > 0, row < lax.axis_size("wide") - 1, col > 0, col < lax.axis_size("narrow") - 1)
    copies[0].wait()
    for face, (base, size) in enumerate(FACES):
        count = counts[0, 0, face]
        slots = lax.broadcasted_iota(jnp.int32, (WIDTH, size), 1)
        live_ref[:, base : base + size] = jnp.where(slots < count, 1.0, 0.0).astype(BF16)
        inner = jnp.where(bounded[face], count, 0)
        inside_ref[:, base : base + size] = jnp.where(slots < inner, 1.0, 0.0).astype(BF16)
    copies[1].wait()
    flipped = lax.dot_general(identity(WIDTH), rows[...], ACROSS, preferred_element_type=F32).astype(BF16)
    kept_ref[...] = flipped
    faces = [flipped[:, base : base + size] for base, size in FACES]
    wf_ref[...], ws_ref[...] = crossed("wide", faces[0], faces[1])
    nf_ref[...], ns_ref[...] = crossed("narrow", faces[2], faces[3])


def turn(operator_ref, out_ref):
    unit = identity(BLOCK)
    for part in range(2):
        for low in range(0, TOTAL, BLOCK):
            for base in range(0, TOTAL, BLOCK):
                tile = operator_ref[0, 0, part, low : low + BLOCK, base : base + BLOCK]
                turned = lax.dot_general(unit, tile, ACROSS, preferred_element_type=F32)
                out_ref[part, base : base + BLOCK, low : low + BLOCK] = turned.astype(BF16)


def received(axis, first_ref, second_ref, mask):
    lower, higher = crossed(axis, first_ref[...], second_ref[...])
    return masked(jnp.concatenate([lower, higher], axis=1), mask)


def terms(op_ref, rows, columns, field):
    turn = jnp.concatenate([-field[HALF:], field[:HALF]], axis=0)
    first = jnp.dot(field, op_ref[0, rows, columns], preferred_element_type=F32)
    return first + jnp.dot(turn, op_ref[1, rows, columns], preferred_element_type=F32)


def from_wide(op_ref, kept_ref, inside_ref, first_ref, second_ref, sum_ref):
    field = received("wide", first_ref, second_ref, inside_ref[:, :WIDE])
    for base in range(0, TOTAL, BLOCK):
        at = slice(base, base + BLOCK)
        sum_ref[:, at] = terms(op_ref, slice(0, WIDE), at, field) + kept_ref[:, at].astype(F32)


def narrow_base(first):
    base = jnp.where(even("narrow") == first, WIDE + FACE_SHORT, WIDE)
    return pl.multiple_of(base, 128)


def narrow_terms(op_ref, base, columns, field):
    turn = jnp.concatenate([-field[HALF:], field[:HALF]], axis=0)
    head, tail = pl.ds(base, BLOCK), pl.ds(pl.multiple_of(base + BLOCK, 128), FACE_SHORT - BLOCK)
    total = jnp.dot(field[:, :BLOCK], op_ref[0, head, columns], preferred_element_type=F32)
    total += jnp.dot(turn[:, :BLOCK], op_ref[1, head, columns], preferred_element_type=F32)
    both = jnp.concatenate([field[:, BLOCK:], turn[:, BLOCK:]], axis=1)
    rest = jnp.concatenate([op_ref[0, tail, columns], op_ref[1, tail, columns]], axis=0)
    return total + jnp.dot(both, rest, preferred_element_type=F32)


def from_first(op_ref, inside_ref, narrow_ref, before_ref, sum_ref):
    base = narrow_base(True)
    side = masked(narrow_ref[...], inside_ref[:, pl.ds(base, FACE_SHORT)])
    for start in range(0, TOTAL, BLOCK):
        at = slice(start, start + BLOCK)
        sum_ref[:, at] = narrow_terms(op_ref, base, at, side) + before_ref[:, at]


def finish(op_ref, live_ref, inside_ref, narrow_ref, sum_ref, outs):
    base = narrow_base(False)
    side = masked(narrow_ref[...], inside_ref[:, pl.ds(base, FACE_SHORT)])
    for out_ref, axis, first in outs:
        low, size = (0, FACE_LONG) if axis == "wide" else (WIDE, FACE_SHORT)
        at = pl.ds(pl.multiple_of(jnp.where(even(axis) == first, low + size, low), 128), size)
        total = narrow_terms(op_ref, base, at, side) + sum_ref[:, at]
        out_ref[...] = masked(total.astype(BF16), live_ref[:, at])


def finish_most(*refs):
    finish(*refs[:5], ((refs[5], "wide", False), (refs[6], "narrow", False), (refs[7], "narrow", True)))


def finish_rest(*refs):
    finish(*refs[:5], ((refs[5], "wide", True),))


def put(out_ref, rows_ref, sems, value):
    unit = identity(BLOCK)
    copies = []
    for i, base in enumerate(range(0, TOTAL, BLOCK)):
        rows = lax.dot_general(unit, value[:, base : base + BLOCK], ACROSS, preferred_element_type=F32)
        rows_ref[base : base + BLOCK] = rows.astype(BF16)
        at = pl.ds(base, BLOCK)
        copies.append(pltpu.make_async_copy(rows_ref.at[at], out_ref.at[0, 0, at], sems.at[i]))
        copies[-1].start()
    for copy in copies:
        copy.wait()


def emit_outgoing(wf_ref, ws_ref, nf_ref, ns_ref, out_ref, rows_ref, sems):
    pieces = crossed("wide", wf_ref[...], ws_ref[...]) + crossed("narrow", nf_ref[...], ns_ref[...])
    put(out_ref, rows_ref, sems, jnp.concatenate(pieces, axis=1))


def emit_incoming(inside_ref, wf_ref, ws_ref, nf_ref, ns_ref, out_ref, rows_ref, sems):
    pieces = crossed("wide", wf_ref[...], ws_ref[...]) + crossed("narrow", nf_ref[...], ns_ref[...])
    put(out_ref, rows_ref, sems, masked(jnp.concatenate(pieces, axis=1), inside_ref[...]))


def body(operator, sources, face_lengths):
    faces = [LONG, LONG, SHORT, SHORT]
    unit = 2 * 2 * WIDTH
    scratch = [pltpu.SMEM((1, 1, 4), jnp.int32), pltpu.VMEM((TOTAL, WIDTH), BF16), pltpu.SemaphoreType.DMA((2,))]
    kept, live, inside, *out = call(prepare, [WHOLE] * 3 + faces, [ANY, ANY], 1 << 34, scratch)(
        stored(face_lengths), stored(sources)
    )
    into = swap_all(out)
    (oper,) = call(turn, [pltpu.VMEM((2, TOTAL, TOTAL), BF16)], [VMEM], 1 << 33)(held(operator))
    oper, kept, live, inside = map(held, (oper, kept, live, inside))
    for _ in range(ITERS):
        wf, ws, nf, ns = map(held, into)
        (total,) = call(
            from_wide, [pltpu.VMEM((WIDTH, TOTAL), F32)], [VMEM] * 5, unit * TOTAL * WIDE
        )(oper, kept, inside, wf, ws)
        (total,) = call(
            from_first, [pltpu.VMEM((WIDTH, TOTAL), F32)], [VMEM] * 4, unit * TOTAL * FACE_SHORT
        )(oper, inside, nf, held(total))
        args, work = (oper, live, inside, ns, held(total)), unit * 1024 * FACE_SHORT
        ws, ns, nf = call(finish_most, [LONG, SHORT, SHORT], [VMEM] * 5, work)(*args)
        (wf,) = call(finish_rest, [LONG], [VMEM] * 5, work)(*args)
        out = [wf, ws, nf, ns]
        into = swap_all(out)
    scratch = [pltpu.VMEM((TOTAL, WIDTH), BF16), pltpu.SemaphoreType.DMA((TOTAL // BLOCK,))]
    result = [jax.ShapeDtypeStruct((1, 1, TOTAL, WIDTH), BF16)]
    (outgoing,) = call(emit_outgoing, result, [VMEM] * 4, 1 << 26, scratch, ANY)(*map(held, out))
    (incoming,) = call(emit_incoming, result, [VMEM] * 5, 1 << 20, scratch, ANY)(inside, *map(held, into))
    return (outgoing, incoming)


def solution(mesh):
    in_specs = (
        P("wide", "narrow", None, None, None),
        P("wide", "narrow", None, None),
        P("wide", "narrow", None),
    )
    out_specs = (P("wide", "narrow", None, None), P("wide", "narrow", None, None))
    return jax.shard_map(body, mesh=mesh, in_specs=in_specs, out_specs=out_specs, check_vma=False)
```
